32 devices in a mesh: dp: 2 (over x), ep: 16 (over z, y, core).
Axes of the slice: x: 2, y: 2, z: 4, core: 2. Of those that a mesh axis runs over, the one named last changes fastest.
Arguments:
- tokens: bfloat16 [256, 3584], P(('dp', 'ep')), may hold values from -6 to 6
- expert_ids: int32 [2, 256, 8], P(None, ('dp', 'ep')), may hold values from 0 to 15, all different within a row; in each aligned block of 8 rows (0 to 7, 8 to 15, ..., all dimensions but the last counted through in order) at most 6 rows name the same one
- quant_gates: int32 [2, 256, 8], P(None, ('dp', 'ep')), may hold values from 1 to 63
- w_gate: bfloat16 [2, 16, 3584, 1024], P(None, 'ep', None, 'dp'), may hold values from -0.09375 to 0.09375
- w_up: bfloat16 [2, 16, 3584, 1024], P(None, 'ep', None, 'dp'), may hold values from -0.09375 to 0.09375
- w_down: bfloat16 [2, 16, 1024, 3584], P(None, 'ep', 'dp'), may hold values from -0.1875 to 0.1875
Outputs:
- stream_out: bfloat16 [256, 3584], P(('dp', 'ep'))
- expert_load: int32 [2, 16], replicated
The draws below stay inside these ranges and needn't reach their ends.
Inputs may be any that keep to these rules, and one draw needn't show every extreme that they name: `expert_ids`: in each layer, the 8 tokens of one device name any one expert at most 6 times, a bound that some block reaches.
All inputs are finite; a program needn't handle non-finite values.
Results may differ from the reference program's by a relative error of at most 0.015.
Values may be sent and summed in bfloat16 or wider, within the bound.
A program may use at most 64 MiB of HBM per device.

```python
import math
import jax
import jax.numpy as jnp
import numpy as np
from jax import lax

D = 3584
FFW = 1024
TOP = 8
LAYERS = 2
TOK_DEV = 8
EXPERTS = 16
CAP = 6
FF_DEV = 512
TOKENS = 256
N_DP = 2
N_EP = 16


def place_ends(values, rng, low, largest):
    place = [jax.random.randint(jax.random.fold_in(rng, axis), (), 0, length) for axis, length in enumerate(values.shape)]
    widest = values.shape.index(max(values.shape))
    neighbour = place[:widest] + [(place[widest] + 1) % values.shape[widest]] + place[widest + 1:]
    return values.at[tuple(place)].set(low).at[tuple(neighbour)].set(largest)


def block_scale(own_key, dims, pieces, low, largest):
    gain = 1.0
    for dim, blocks in pieces:
        draws = jax.random.uniform(jax.random.fold_in(jax.random.fold_in(own_key, 6), dim), (blocks,), jnp.float32, low / len(pieces), largest / len(pieces))
        gain = gain * jnp.repeat(jnp.exp(draws), dims[dim] // blocks).reshape((-1,) + (1,) * (len(dims) - 1 - dim))
    return gain


def shared_out(own_key, own, number, rows, number_of, top, limit, slope):
    sequence = jax.random.permutation(own_key, number_of)
    packed, ordinary = load_shares(number_of, rows * top, limit, slope, True), load_shares(number_of, rows * top, limit, slope, False)
    places = jnp.arange(number_of)

    def named(lengths, rotation):
        used = int((lengths > 0).sum())
        fixed = max(1, used // 4)
        moved = fixed + (places - fixed + rotation * (used - fixed)) % max(1, number_of - fixed)
        return jnp.zeros((number_of,), jnp.int32).at[sequence[jnp.where(places < fixed, places, moved)]].set(jnp.asarray(lengths, jnp.int32))

    lengths = jnp.where(number % 4 == 0, named(packed, number // 4), named(ordinary, number - number // 4 - 1))
    mixed = jax.random.permutation(jax.random.fold_in(own, 3), number_of)
    donor, taker = mixed[0:number_of // 2 * 2:2], mixed[1:number_of // 2 * 2:2]
    room = jnp.minimum(lengths[donor] - 1, limit - lengths[taker]) // 2
    room = jnp.where((donor == sequence[0]) | (taker == sequence[0]) | (lengths[taker] == 0), 0, jnp.maximum(room, 0))
    moved = jax.random.randint(jax.random.fold_in(own, 4), (number_of // 2,), 0, 1 << 20) % (room + 1)
    lengths = lengths.at[donor].add(-moved).at[taker].add(moved)
    members = jnp.searchsorted(jnp.cumsum(lengths), jnp.arange(rows * top), side="right").astype(jnp.int32)
    table = members.reshape(top, rows).T
    table = table[jax.random.permutation(jax.random.fold_in(own, 1), rows)]
    rotation = jax.random.randint(jax.random.fold_in(own, 2), (rows, 1), 0, top)
    return jnp.take_along_axis(table, (jnp.arange(top)[None, :] + rotation) % top, axis=1)


def load_shares(number_of, total, reach, lean, full):
    weights = [(1 << 20) // math.isqrt(standing ** lean) + 1 for standing in range(1, number_of + 1)]
    largest = reach if full else min(reach, max(-(-total // number_of), total * weights[0] // sum(weights)))
    least = 1 if total - largest >= number_of - 1 else 0
    given, spare = [largest] + [least] * (number_of - 1), total - largest - least * (number_of - 1)
    while spare > 0:
        free = [i for i in range(1, number_of) if given[i] < largest] or [i for i in range(1, number_of) if given[i] < reach]
        whole, budget = sum([weights[i] for i in free]), spare
        for i in free:
            extra = min(reach - given[i], max(1, budget * weights[i] // whole), spare)
            given[i] = given[i] + extra
            spare = spare - extra
    return np.array(given)


def bell_draw(stream_key, extent, scale, most, shards=(), dtype=jnp.bfloat16):
    factor_of = block_scale(stream_key, extent, shards, -0.22, 0.18) if shards else 1.0
    drawn = jax.random.normal(stream_key, extent, jnp.float32) * scale * factor_of
    return jnp.minimum(jnp.maximum(drawn, -most), most).astype(dtype)


def setup_inputs(seed: int = 0) -> dict:
    key_list = jax.random.split(jax.random.key(seed), 7)
    tokens = bell_draw(key_list[0], (TOKENS, D), 1.0, 6.0, ((0, 32),))
    expert_ids_keys = jax.random.split(jax.random.fold_in(key_list[1], 1), LAYERS * TOKENS // TOK_DEV)
    expert_ids_turns = jax.random.permutation(jax.random.fold_in(key_list[1], 3), LAYERS * TOKENS // TOK_DEV)
    expert_ids = jax.vmap(lambda own, number: shared_out(jax.random.fold_in(key_list[1], 2), own, number, TOK_DEV, EXPERTS, TOP, CAP, 2))(expert_ids_keys, expert_ids_turns).reshape((LAYERS, TOKENS, TOP))
    quant_gates = place_ends(jax.random.randint(key_list[2], (LAYERS, TOKENS, TOP), 1, 64), jax.random.fold_in(key_list[2], 1), 1, 63).astype(jnp.int32)
    w_gate = bell_draw(key_list[3], (LAYERS, EXPERTS, D, FFW), D ** -0.5, 0.09375, ((1, 16), (3, 2)))
    w_up = bell_draw(key_list[4], (LAYERS, EXPERTS, D, FFW), D ** -0.5, 0.09375, ((1, 16), (3, 2)))
    w_down = bell_draw(key_list[5], (LAYERS, EXPERTS, FFW, D), FFW ** -0.5, 0.1875, ((1, 16), (2, 2)))
    return dict(tokens=tokens, expert_ids=expert_ids, quant_gates=quant_gates, w_gate=w_gate, w_up=w_up, w_down=w_down)


ROUTE_SCALE = 2.827
EPS = 1e-06

def expert_rows(rows, weight_gate, weight_up, weight_down):
    gate = jnp.dot(rows, weight_gate, preferred_element_type=jnp.float32)
    upper = jnp.dot(rows, weight_up, preferred_element_type=jnp.float32)
    hidden = (jax.nn.silu(gate) * upper).astype(jnp.bfloat16)
    total = jnp.zeros((rows.shape[0], D), jnp.float32)
    for block in range(N_DP):
        lower_edge = block * FF_DEV
        piece = jnp.dot(hidden[:, lower_edge:lower_edge + FF_DEV], weight_down[lower_edge:lower_edge + FF_DEV], preferred_element_type=jnp.float32)
        total = total + piece.astype(jnp.bfloat16).astype(jnp.float32)
    return total

def reference(tokens, expert_ids, quant_gates, w_gate, w_up, w_down):
    state = tokens
    most_rows = CAP * N_DP * N_EP
    loads = []
    for layer in range(LAYERS):
        wide = state.astype(jnp.float32)
        normed = (wide * lax.rsqrt(lax.optimization_barrier(jnp.mean(wide * wide, axis=1, keepdims=True)) + EPS)).astype(jnp.bfloat16)
        flat_ids = expert_ids[layer].reshape(TOKENS * TOP).astype(jnp.int32)
        quant = quant_gates[layer].astype(jnp.float32)
        gates = (ROUTE_SCALE * quant / lax.optimization_barrier(jnp.sum(quant, axis=1, keepdims=True))).reshape(TOKENS * TOP)
        expert_iota = lax.broadcasted_iota(jnp.int32, (1, EXPERTS), 1)
        loads.append(lax.optimization_barrier(jnp.sum((flat_ids[:, None] == expert_iota).astype(jnp.int32), axis=0)).astype(jnp.int32))

        def one_expert(expert, accum):
            order = jnp.argsort((flat_ids != expert).astype(jnp.int32), stable=True)[:most_rows].astype(jnp.int32)
            valid = flat_ids[order] == expert
            token_index = (order // TOP).astype(jnp.int32)
            rows = normed[token_index]
            result = expert_rows(rows, w_gate[layer, expert], w_up[layer, expert], w_down[layer, expert])
            weight = jnp.where(valid, gates[order], jnp.float32(0.0))
            return accum.at[token_index].add(weight[:, None] * result)
        branch = lax.fori_loop(0, EXPERTS, one_expert, jnp.zeros((TOKENS, D), jnp.float32))
        state = (state.astype(jnp.float32) + branch).astype(jnp.bfloat16)
    return (state, jnp.stack(loads))
```

```python
import functools

import jax
import jax.numpy as jnp
from jax import lax
from jax.experimental import pallas as pl
from jax.experimental.pallas import tpu as pltpu
from jax.sharding import PartitionSpec as P

ROUTE_SCALE = 2.827
EPS = 1e-06


def slot_tables(ids, quant, experts, capacity):
    count_tok, top = ids.shape
    flat = ids.reshape(count_tok * top)
    expert_iota = lax.broadcasted_iota(jnp.int32, (count_tok * top, experts), 1)
    onehot = (flat[:, None] == expert_iota).astype(jnp.int32)
    earlier = jnp.cumsum(onehot, axis=0) - onehot
    position = jnp.sum(earlier * onehot, axis=1)
    target = flat * capacity + position
    slot_iota = lax.broadcasted_iota(jnp.int32, (count_tok * top, experts * capacity), 1)
    picked = target[:, None] == slot_iota
    quant_wide = quant.astype(jnp.float32)
    gates = (ROUTE_SCALE * quant_wide / jnp.sum(quant_wide, axis=1, keepdims=True)).reshape(
        count_tok * top
    )
    spread = jnp.sum(
        jnp.where(picked, gates[:, None], 0.0).reshape(count_tok, top, experts * capacity), axis=1
    )
    chosen = jnp.sum(picked.astype(jnp.float32).reshape(count_tok, top, experts * capacity), axis=1)
    counts = jnp.sum(onehot, axis=0)
    return (chosen, spread, counts)


def per_device(tokens, expert_ids, quant_gates, w_gate, w_up, w_down):
    layers, count_tok, top = expert_ids.shape
    n_ep = lax.axis_size("ep")
    capacity = min(count_tok, max(2, 3 * count_tok * top // (2 * n_ep)))
    width = tokens.shape[1]
    state = tokens
    table = jnp.stack(
        [
            slot_tables(expert_ids[layer], quant_gates[layer], n_ep, capacity)[2]
            for layer in range(layers)
        ]
    )
    loads = lax.psum(table, ("dp", "ep"))
    for layer in range(layers):
        chosen, spread, counts = slot_tables(expert_ids[layer], quant_gates[layer], n_ep, capacity)
        wide = state.astype(jnp.float32)
        normed = (wide * lax.rsqrt(jnp.mean(wide * wide, axis=1, keepdims=True) + EPS)).astype(
            jnp.bfloat16
        )
        outgoing = jnp.dot(
            chosen.T.astype(jnp.bfloat16), normed, preferred_element_type=jnp.float32
        ).astype(jnp.bfloat16)
        arrived = lax.all_to_all(
            outgoing.reshape(n_ep, capacity, width), "ep", split_axis=0, concat_axis=0, tiled=True
        )
        arrived = arrived.reshape(n_ep * capacity, width)
        weight_gate = w_gate[layer, 0]
        weight_up = w_up[layer, 0]
        weight_down = w_down[layer, 0]
        piece = lax.all_gather(arrived, "dp", axis=0, tiled=True)
        gate = jnp.dot(piece, weight_gate, preferred_element_type=jnp.float32)
        upper = jnp.dot(piece, weight_up, preferred_element_type=jnp.float32)
        hidden = (jax.nn.silu(gate) * upper).astype(jnp.bfloat16)
        partial_out = jnp.dot(hidden, weight_down, preferred_element_type=jnp.float32)
        parts = partial_out.astype(jnp.bfloat16)
        summed = lax.psum_scatter(
            parts.astype(jnp.float32).astype(jnp.bfloat16), "dp", scatter_dimension=0, tiled=True
        ).astype(jnp.float32)
        returned = lax.all_to_all(
            summed.reshape(n_ep, capacity, width).astype(jnp.bfloat16),
            "ep",
            split_axis=0,
            concat_axis=0,
            tiled=True,
        ).astype(jnp.float32)
        branch = jnp.dot(
            spread,
            returned.reshape(n_ep * capacity, width),
            precision=lax.Precision.HIGHEST,
            preferred_element_type=jnp.float32,
        )
        state = (state.astype(jnp.float32) + branch).astype(jnp.bfloat16)
    return (state, loads)


MESH = pl.DeviceIdType.MESH
LANES = 128
VMEM_BYTES = 60 * 1024 * 1024


def moe_kernel(
    n_z, x_ref, ids_ref, quant_ref, wg_hbm, wu_hbm, wd_hbm, out_ref, load_ref,
    wg, wu, wd, mine, theirs, xown, xpar, state, hid, yown, ysend, r0, s1, r1, s2, r2, s3, r3,
    sq_send, sq_recv, f_send, f_recv,
    w_sem, first_sem, sq_sem, f_sem, ag_send, ag_recv, dd_send, dd_recv, y_send, y_recv,
    s1_send, s1_recv, s2_send, s2_recv, s3_send, s3_recv,
):
    layers, tok, top = ids_ref.shape
    width = x_ref.shape[1]
    half = width // 2
    ff = wg.shape[2]
    chip = 2 * tok
    dx = lax.axis_index("dp")
    ep = lax.axis_index("ep")
    c = ep % 2
    b = (ep // 2) % 2
    a = ep // 4
    n_ep = 4 * n_z
    own0 = pl.multiple_of(c * half, LANES)
    par0 = pl.multiple_of((1 - c) * half, LANES)

    def device(za, yb, xd, core):
        return (xd, (za * 2 + yb) * 2 + core)

    def block(za, yb, xd):
        return (za * 2 + yb) * 2 + xd

    def rows(blk):
        return pl.ds(pl.multiple_of(blk * chip, chip), chip)

    b1, x1 = (b + c) % 2, (dx + 1 - c) % 2
    b2, x2 = (b + 1 - c) % 2, (dx + c) % 2
    b3, x3 = 1 - b, 1 - dx
    peer = device(a, b, dx, 1 - c)
    p1 = device(a, b1, x1, c)
    p2 = device(a, b2, x2, c)
    order = [d for d in range(1, n_z)]
    zs = [(a + d) % n_z for d in range(n_z)]

    loads = []
    for l in range(layers):
        for i, (src, dst) in enumerate(((wg_hbm, wg), (wu_hbm, wu), (wd_hbm, wd))):
            copy = pltpu.make_async_copy(src.at[l, 0], dst.at[l], w_sem.at[l, i])
            copy.start()
            loads.append(copy)

    barrier = pltpu.get_barrier_semaphore()
    targets = [peer, p1, p2] + [device(zs[d], b, dx, c) for d in order]
    for target in targets:
        pl.semaphore_signal(barrier, inc=1, device_id=target, device_id_type=MESH)

    lane = lax.broadcasted_iota(jnp.int32, (tok, LANES), 1)
    table = jnp.zeros((tok, LANES), jnp.float32)
    for l in range(layers):
        ids = ids_ref[l]
        quant = quant_ref[l].astype(jnp.float32)
        for k in range(top):
            table += jnp.where(lane == ids[:, k : k + 1] + l * n_ep, quant[:, k : k + 1], 0.0)
    mine[:, :width] = x_ref[...].astype(jnp.float32)
    mine[:, width:] = table
    pl.semaphore_wait(barrier, len(targets))

    def remote(src, dst, send, recv, target):
        return pltpu.make_async_remote_copy(
            src_ref=src, dst_ref=dst, send_sem=send, recv_sem=recv, device_id=target, device_id_type=MESH
        )

    swap = remote(mine, theirs, first_sem.at[0], first_sem.at[1], peer)
    swap.start()
    swap.wait()

    def by_core(own, other):
        return jnp.concatenate(
            [jnp.where(c == 0, own, other), jnp.where(c == 0, other, own)], axis=0
        )

    my_block = block(a, b, dx)
    pairs = by_core(mine[:, width:], theirs[:, width:])
    total = jnp.sum(mine[:, :width] * mine[:, :width], axis=1, keepdims=True)
    total_other = jnp.sum(theirs[:, :width] * theirs[:, :width], axis=1, keepdims=True)
    square = by_core(total, total_other)
    state[...] = by_core(mine[:, pl.ds(own0, half)], theirs[:, pl.ds(own0, half)])

    for l in range(layers):
        if l > 0:
            part = jnp.sum(state[...] * state[...], axis=1, keepdims=True)
            sq_send[l] = jnp.broadcast_to(part, (chip, LANES))
            swap = remote(sq_send.at[l], sq_recv.at[l], sq_sem.at[l, 0], sq_sem.at[l, 1], peer)
            swap.start()
            swap.wait()
            square = (sq_send[l] + sq_recv[l])[:, :1]
        normed = state[...] * lax.rsqrt(square / width + EPS)
        xown[l, rows(my_block), :half] = normed.astype(jnp.bfloat16)
        if l == 0:
            xown[l, rows(my_block), half:] = pairs.astype(jnp.bfloat16)
        cols = slice(0, half + LANES) if l == 0 else slice(0, half)
        pending = []
        slot = [0]

        def forward(blk, target):
            ref = xown.at[l, rows(blk), cols]
            copy = remote(ref, ref, ag_send.at[l, slot[0]], ag_recv.at[l, blk], target)
            copy.start()
            slot[0] += 1
            pending.append(copy)

        def across(blk):
            copy = remote(
                xown.at[l, rows(blk), slice(0, half)], xpar.at[l, rows(blk)],
                dd_send.at[l, blk], dd_recv.at[l, blk], peer,
            )
            copy.start()
            pending.append(copy)

        def arrived(blk):
            ref = xown.at[l, rows(blk), cols]
            remote(ref, ref, ag_send.at[l, 0], ag_recv.at[l, blk], p1).wait_recv()

        for d in order:
            forward(my_block, device(zs[d], b, dx, c))
        forward(my_block, p1)
        forward(my_block, p2)
        across(my_block)
        blk = block(a, b1, x1)
        arrived(blk)
        forward(blk, p2)
        across(blk)
        for d in order:
            blk = block(zs[d], b, dx)
            arrived(blk)
            forward(blk, p1)
            forward(blk, p2)
            across(blk)
        for d in order:
            blk = block(zs[d], b1, x1)
            arrived(blk)
            forward(blk, p2)
            across(blk)
        for d in range(n_z):
            for blk in (block(zs[d], b2, x2), block(zs[d], b3, x3)):
                arrived(blk)
                across(blk)
        for blk in range(4 * n_z):
            ref = xpar.at[l, rows(blk)]
            remote(ref, ref, dd_send.at[l, blk], dd_recv.at[l, blk], peer).wait_recv()
        for copy in pending:
            copy.wait_send()
        for copy in loads[3 * l : 3 * l + 3]:
            copy.wait()

        count = 4 * n_z * chip
        score = xown[0, :, half:].astype(jnp.float32)
        wide_lane = lax.broadcasted_iota(jnp.int32, (count, LANES), 1)
        here = jnp.sum(jnp.where(wide_lane == l * n_ep + ep, score, 0.0), axis=1, keepdims=True)
        every = jnp.sum(
            jnp.where((wide_lane >= l * n_ep) & (wide_lane < (l + 1) * n_ep), score, 0.0),
            axis=1, keepdims=True,
        )
        gate_row = ROUTE_SCALE * here / every
        if l == 0:
            seen = jnp.sum((score > 0.0).astype(jnp.float32), axis=0, keepdims=True).astype(jnp.int32)
            for m in range(layers):
                load_ref[m : m + 1, :] = seen[:, m * n_ep : (m + 1) * n_ep]

        tile = 256

        def expand(j, _):
            col = pl.ds(pl.multiple_of(j * tile, tile), tile)

            def product(weight):
                return jnp.dot(
                    xown[l, :, :half], weight[l, pl.ds(own0, half), col], preferred_element_type=jnp.float32
                ) + jnp.dot(xpar[l], weight[l, pl.ds(par0, half), col], preferred_element_type=jnp.float32)

            gate = product(wg)
            upper = product(wu)
            hid[:, col] = (jax.nn.silu(gate) * upper).astype(jnp.bfloat16)
            return 0

        lax.fori_loop(0, ff // tile, expand, 0)

        def down(base, j):
            return gate_row * jnp.dot(
                hid[...], wd[l, :, pl.ds(pl.multiple_of(base + j * tile, LANES), tile)],
                preferred_element_type=jnp.float32,
            )

        def crossing(j):
            col = pl.ds(pl.multiple_of(j * tile, tile), tile)
            return remote(ysend.at[l, :, col], r0.at[l, :, col], y_send.at[l, j], y_recv.at[l, j], peer)

        def down_par(j, _):
            ysend[l, :, pl.ds(pl.multiple_of(j * tile, tile), tile)] = down(par0, j).astype(jnp.bfloat16)
            crossing(j).start()
            return 0

        def down_own(j, _):
            yown[:, pl.ds(pl.multiple_of(j * tile, tile), tile)] = down(own0, j)
            return 0

        lax.fori_loop(0, half // tile, down_par, 0)
        lax.fori_loop(0, half // tile, down_own, 0)
        for j in range(half // tile):
            crossing(j).wait()

        def local(blk):
            return yown[rows(blk), :] + r0[l, rows(blk), :].astype(jnp.float32)

        def part_of(k):
            return pl.ds(k * chip, chip)

        turn = order + [0]
        sends = []
        for d in turn:
            for q, (yb, xd) in enumerate(((b3, x3), (b2, x2))):
                k = 2 * d + q
                s1[l, part_of(k), :] = local(block(zs[d], yb, xd)).astype(jnp.bfloat16)
                copy = remote(
                    s1.at[l, part_of(k)], r1.at[l, part_of(k)], s1_send.at[l, k], s1_recv.at[l, k], p2
                )
                copy.start()
                sends.append(copy)

        def got(buf, k, send, recv):
            ref = buf.at[l, part_of(k)]
            remote(ref, ref, send.at[l, k], recv.at[l, k], p1).wait_recv()
            return buf[l, part_of(k), :].astype(jnp.float32)

        def second(d):
            s2[l, part_of(d), :] = (
                local(block(zs[d], b1, x1)) + got(r1, 2 * d, s1_send, s1_recv)
            ).astype(jnp.bfloat16)
            copy = remote(s2.at[l, part_of(d)], r2.at[l, part_of(d)], s2_send.at[l, d], s2_recv.at[l, d], p1)
            copy.start()
            sends.append(copy)

        def third(d):
            value = (
                local(block(zs[d], b, dx))
                + got(r1, 2 * d + 1, s1_send, s1_recv)
                + got(r2, d, s2_send, s2_recv)
            )
            if d == 0:
                return value
            s3[l, part_of(d), :] = value.astype(jnp.bfloat16)
            copy = remote(
                s3.at[l, part_of(d)], r3.at[l, part_of(d)], s3_send.at[l, d], s3_recv.at[l, d],
                device(zs[d], b, dx, c),
            )
            copy.start()
            sends.append(copy)
            return None

        for i, d in enumerate(turn):
            second(d)
            if i > 0:
                third(turn[i - 1])
        branch = third(0)
        for d in order:
            branch = branch + got(r3, d, s3_send, s3_recv)
        state[...] = (state[...] + branch).astype(jnp.bfloat16).astype(jnp.float32)
        for copy in sends:
            copy.wait_send()

    low, high = state[:tok, :], state[tok:, :]
    f_send[...] = jnp.where(c == 0, high, low)
    swap = remote(f_send, f_recv, f_sem.at[0], f_sem.at[1], peer)
    swap.start()
    out_ref[:, pl.ds(own0, half)] = jnp.where(c == 0, low, high).astype(out_ref.dtype)
    swap.wait()
    out_ref[:, pl.ds(par0, half)] = f_recv[...].astype(out_ref.dtype)


def scratch_list(n_z, layers, tok, width, ff):
    half, chip = width // 2, 2 * tok
    count = 4 * n_z * chip
    blocks = 4 * n_z
    bf16, f32 = jnp.bfloat16, jnp.float32
    buffers = [
        ((layers, width, ff), bf16),
        ((layers, width, ff), bf16),
        ((layers, ff, width), bf16),
        ((tok, width + LANES), f32),
        ((tok, width + LANES), f32),
        ((layers, count, half + LANES), bf16),
        ((layers, count, half), bf16),
        ((chip, half), f32),
        ((count, ff), bf16),
        ((count, half), f32),
        ((layers, count, half), bf16),
        ((layers, count, half), bf16),
        ((layers, count // 2, half), bf16),
        ((layers, count // 2, half), bf16),
        ((layers, count // 4, half), bf16),
        ((layers, count // 4, half), bf16),
        ((layers, count // 4, half), bf16),
        ((layers, count // 4, half), bf16),
        ((layers, chip, LANES), f32),
        ((layers, chip, LANES), f32),
        ((tok, half), f32),
        ((tok, half), f32),
    ]
    sems = [
        (layers, 3), (2,), (layers, 2), (2,),
        (layers, blocks), (layers, blocks), (layers, blocks), (layers, blocks),
        (layers, max(1, half // 256)), (layers, max(1, half // 256)),
        (layers, 2 * n_z), (layers, 2 * n_z), (layers, n_z), (layers, n_z), (layers, n_z), (layers, n_z),
    ]
    size = 0
    for shape, dtype in buffers:
        bytes_of = jnp.dtype(dtype).itemsize
        for dim in shape:
            bytes_of *= dim
        size += bytes_of
    return buffers, sems, size


def fused_device(n_z, tokens, expert_ids, quant_gates, w_gate, w_up, w_down):
    layers, tok, _ = expert_ids.shape
    width = tokens.shape[1]
    ff = w_gate.shape[3]
    buffers, sems, _ = scratch_list(n_z, layers, tok, width, ff)
    vmem = pl.BlockSpec(memory_space=pltpu.VMEM)
    hbm = pl.BlockSpec(memory_space=pl.ANY)
    out, loads = pl.pallas_call(
        functools.partial(moe_kernel, n_z),
        out_shape=(
            jax.ShapeDtypeStruct((tok, width), tokens.dtype),
            jax.ShapeDtypeStruct((layers, 4 * n_z), jnp.int32),
        ),
        in_specs=[vmem, vmem, vmem, hbm, hbm, hbm],
        out_specs=(vmem, vmem),
        scratch_shapes=[pltpu.VMEM(shape, dtype) for shape, dtype in buffers]
        + [pltpu.SemaphoreType.DMA(shape) for shape in sems],
        compiler_params=pltpu.CompilerParams(
            collective_id=0, has_side_effects=True, vmem_limit_bytes=VMEM_BYTES
        ),
    )(tokens, expert_ids, quant_gates, w_gate, w_up, w_down)
    return (out, loads)


def solution(mesh):
    n_dp, n_ep = mesh.shape["dp"], mesh.shape["ep"]

    def step(tokens, expert_ids, quant_gates, w_gate, w_up, w_down):
        layers, tok, _ = expert_ids.shape
        width, ff = tokens.shape[1], w_gate.shape[3]
        fits = (
            n_dp == 2 and n_ep % 4 == 0 and n_ep > 4 and tok == 8 and width % 512 == 0
            and ff % 256 == 0 and layers * n_ep <= LANES
        )
        if fits and scratch_list(n_ep // 4, layers, tok, width, ff)[2] < VMEM_BYTES * 4 // 5:
            return fused_device(n_ep // 4, tokens, expert_ids, quant_gates, w_gate, w_up, w_down)
        return per_device(tokens, expert_ids, quant_gates, w_gate, w_up, w_down)

    return jax.shard_map(
        step,
        mesh=mesh,
        in_specs=(
            P(("dp", "ep"), None),
            P(None, ("dp", "ep"), None),
            P(None, ("dp", "ep"), None),
            P(None, "ep", None, "dp"),
            P(None, "ep", None, "dp"),
            P(None, "ep", "dp", None),
        ),
        out_specs=(P(("dp", "ep"), None), P()),
        check_vma=False,
    )
```
